256 devices in a mesh: seq: 64 (over x_hi, z, y), tp: 4 (over x_lo, core).
Axes of the slice: x: 4 (x_hi: 2, x_lo: 2; x = x_hi * 2 + x_lo), y: 4, z: 8, core: 2. Of those that a mesh axis runs over, the one named last changes fastest.
Arguments:
- queries: bfloat16 [1, 16384, 4096], P(None, 'seq', 'tp'), may hold values from -13 to 13
- key_rows: bfloat16 [1, 16384, 2048], P(None, 'seq', 'tp'), may hold values from -13 to 13
- value_rows: bfloat16 [1, 16384, 2048], P(None, 'seq', 'tp'), may hold values from -6 to 6
- residual: bfloat16 [1, 16384, 3584], P(None, 'seq', 'tp'), may hold values from -6 to 6
- out_weight: bfloat16 [4096, 3584], P('tp')
- post_scale: float32 [3584], P('tp'), may hold values from 0.1 to 1.9
- lengths: int32 [1], replicated, may hold values from 1024 to 4095
- owners: int32 [1, 64], replicated, may hold values from 0 to 63, each once within a row
Outputs:
- hidden_out: bfloat16 [1, 16384, 3584], P(None, 'seq', 'tp')
- cache_keys: bfloat16 [1, 4096, 2048], P(None, 'seq', 'tp')
- cache_values: bfloat16 [1, 4096, 2048], P(None, 'seq', 'tp')
The draws below stay inside these ranges and needn't reach their ends.
Inputs may be any that keep to these rules, and one draw needn't show every extreme that they name: Each row of owners names every number from 0 to 63 once.
All inputs are finite; a program needn't handle non-finite values.
Results may differ from the reference program's by a relative error of at most 0.0083.
Values may be sent and summed in bfloat16 or wider, within the bound.
No kernel may reach another device: no remote copies, remote signals or barrier semaphores. Data moves between devices by JAX's collectives and lax.ppermute only.
A program may use at most 64 MiB of HBM per device.

```python
import jax
import jax.numpy as jnp
from jax import lax

D = 3584
QH = 16
KVH = 8
HD = 256
WINDOW = 4096
SEQS = 1
SHARD = 256
LENGTH = 16384
N_SEQ = 64


def draw_out_weight(key, part):
    entry_key, jitter_key = jax.random.split(jax.random.fold_in(key, 17))
    fan_in = QH * HD
    entries = jax.random.normal(entry_key, (fan_in, D), jnp.float32)
    rising = jnp.exp(jnp.linspace(jnp.log(0.5), jnp.log(5.0), D)).astype(jnp.float32)
    jitter = jnp.exp(jax.random.uniform(jitter_key, (D,), jnp.float32, -0.35, 0.35))
    return (entries * (rising * jitter)[None, :] * fan_in ** (-0.5)).astype(jnp.bfloat16)


def planted_lift(key):
    mask_key, scale_key, sign_key = jax.random.split(jax.random.fold_in(key, 29), 3)
    fraction = 0.03
    chosen = jax.random.bernoulli(mask_key, fraction, (SEQS, LENGTH))
    amplitude = jax.random.uniform(scale_key, (SEQS, LENGTH), jnp.float32, 8.0, 13.5) * HD ** 0.25
    raised = jnp.where(chosen, amplitude, jnp.zeros_like(amplitude))
    directions = jax.random.rademacher(sign_key, (KVH, HD), jnp.float32) * HD ** (-0.5)
    return (raised, directions)


def background_rows(noise_key, width):
    background = jnp.clip(jax.random.normal(noise_key, (SEQS, LENGTH, width), jnp.float32), -6.0, 6.0)
    return background


def draw_queries(key, part):
    raised, directions = planted_lift(key)
    background = background_rows(jax.random.fold_in(key, 31), QH * HD)
    repeated = jnp.repeat(directions, QH // KVH, axis=0).reshape(QH * HD)
    return (background + raised[:, :, None] * repeated[None, None, :]).astype(jnp.bfloat16)


def draw_key_rows(key, part):
    raised, directions = planted_lift(key)
    background = background_rows(jax.random.fold_in(key, 37), KVH * HD)
    flattened = directions.reshape(KVH * HD)
    return (background + raised[:, :, None] * flattened[None, None, :]).astype(jnp.bfloat16)


def shard_levels(stream_key, dims, shards, smallest, high):
    def one(dim, parts):
        heights = jax.random.uniform(jax.random.fold_in(jax.random.fold_in(stream_key, 6), dim), (parts,), jnp.float32, smallest / len(shards), high / len(shards))
        return jnp.repeat(jnp.exp(heights), dims[dim] // parts).reshape((-1,) + (1,) * (len(dims) - dim - 1))

    loudness = one(*shards[0])
    for cut in shards[1:]:
        loudness = loudness * one(*cut)
    return loudness


def scatter_about(own_key, extent, scale, most, pieces=(), kind=jnp.bfloat16):
    loudness = shard_levels(own_key, extent, pieces, -0.22, 0.18) if pieces else 1.0
    values = jax.random.normal(own_key, extent, jnp.float32) * scale * loudness
    return jnp.minimum(jnp.maximum(values, -most), most).astype(kind)


def setup_inputs(seed: int = 0) -> dict:
    keys = jax.random.split(jax.random.key(seed), 9)
    queries = draw_queries(jax.random.fold_in(keys[8], 71), 0)
    key_rows = draw_key_rows(jax.random.fold_in(keys[8], 71), 0)
    value_rows = scatter_about(keys[2], (SEQS, LENGTH, KVH * HD), 1.0, 6.0, ((1, 64), (2, 4)))
    residual = scatter_about(keys[3], (SEQS, LENGTH, D), 1.0, 6.0, ((1, 64), (2, 4)))
    out_weight = draw_out_weight(jax.random.fold_in(keys[8], 71), 0)
    post_scale = jnp.clip(1.0 + 0.18 * jax.random.normal(keys[5], (D,), jnp.float32), 0.1, 1.9)
    lengths = jax.random.randint(keys[6], (SEQS,), min(WINDOW, LENGTH) // 4, min(WINDOW, LENGTH)).astype(jnp.int32)
    owners = jax.vmap(lambda own: jax.random.permutation(own, N_SEQ))(jax.random.split(keys[7], SEQS)).reshape((SEQS, N_SEQ)).astype(jnp.int32)
    return {"queries": queries, "key_rows": key_rows, "value_rows": value_rows, "residual": residual, "out_weight": out_weight, "post_scale": post_scale, "lengths": lengths, "owners": owners}


soft_cap = 50.0
norm_eps = 1e-06

def attend_rows(queries, padded_keys, padded_values, row_start):
    group_size = QH // KVH
    query_block = lax.dynamic_slice_in_dim(queries, row_start, SHARD, 1).astype(jnp.float32).reshape(SEQS, SHARD, KVH, group_size, HD)
    key_block = lax.dynamic_slice_in_dim(padded_keys, row_start, WINDOW + SHARD, 1).astype(jnp.float32).reshape(SEQS, WINDOW + SHARD, KVH, HD)
    value_block = lax.dynamic_slice_in_dim(padded_values, row_start, WINDOW + SHARD, 1).astype(jnp.float32).reshape(SEQS, WINDOW + SHARD, KVH, HD)
    scores = jnp.einsum('sqhgd,skhd->shgqk', query_block, key_block) * HD ** (-0.5)
    capped = soft_cap * jnp.tanh(scores / soft_cap)
    query_pos = row_start + jnp.arange(SHARD, dtype=jnp.int32)
    key_pos = row_start - WINDOW + jnp.arange(WINDOW + SHARD, dtype=jnp.int32)
    spread = query_pos[:, None] - key_pos[None, :]
    live_mask = (spread >= 0) & (spread < WINDOW) & (key_pos[None, :] >= 0)
    weights = jnp.where(live_mask, jnp.exp(capped), jnp.zeros_like(capped))
    totals = lax.optimization_barrier(jnp.sum(weights, axis=-1))
    rounded = lax.optimization_barrier(weights.astype(jnp.bfloat16)).astype(jnp.float32)
    mixture = jnp.einsum('shgqk,skhd->sqhgd', rounded, value_block)
    attended = mixture / jnp.transpose(totals, (0, 3, 1, 2))[..., None]
    return attended.astype(jnp.bfloat16).reshape(SEQS, SHARD, QH * HD)

def window_rows(rows_in, length):
    slots = jnp.arange(WINDOW, dtype=jnp.int32)
    anchor = length - WINDOW + jnp.mod(slots - length + WINDOW, WINDOW)
    taken = jnp.take(rows_in, jnp.clip(anchor, 0, LENGTH - 1), axis=0)
    return jnp.where((anchor >= 0)[:, None], taken, jnp.zeros_like(taken))

def owner_layout(slotted, owner_row):
    devices = jnp.arange(N_SEQ, dtype=jnp.int32)
    matches = owner_row[:, None] == devices[None, :]
    inverse = lax.optimization_barrier(jnp.sum(jnp.where(matches, devices[:, None], jnp.zeros_like(devices)[:, None]), axis=0))
    local = jnp.arange(WINDOW // N_SEQ, dtype=jnp.int32)
    block_rows = SHARD // N_SEQ
    chosen = local[None, :] // block_rows * SHARD + inverse[:, None] * block_rows + local[None, :] % block_rows
    return jnp.take(slotted, chosen.reshape(-1), axis=0)

def reference(queries, key_rows, value_rows, residual, out_weight, post_scale, lengths, owners):
    front = jnp.zeros((SEQS, WINDOW, KVH * HD), key_rows.dtype)
    padded_keys = jnp.concatenate([front, key_rows], axis=1)
    padded_values = jnp.concatenate([front, value_rows], axis=1)
    starts = jnp.arange(LENGTH // SHARD, dtype=jnp.int32) * SHARD
    blocks = lax.map(lambda row_start: attend_rows(queries, padded_keys, padded_values, row_start), starts)
    attended = jnp.transpose(blocks, (1, 0, 2, 3)).reshape(SEQS * LENGTH, QH * HD)
    branch = jnp.dot(attended, out_weight, preferred_element_type=jnp.float32)
    mean_square = lax.optimization_barrier(jnp.mean(branch * branch, axis=-1, keepdims=True))
    normed = branch * lax.rsqrt(mean_square + norm_eps) * post_scale
    hidden_out = (residual.reshape(SEQS * LENGTH, D).astype(jnp.float32) + normed).astype(jnp.bfloat16).reshape(SEQS, LENGTH, D)
    cache_keys = jnp.stack([owner_layout(window_rows(key_rows[seq_index], lengths[seq_index]), owners[seq_index]) for seq_index in range(SEQS)])
    cache_values = jnp.stack([owner_layout(window_rows(value_rows[seq_index], lengths[seq_index]), owners[seq_index]) for seq_index in range(SEQS)])
    return (hidden_out, cache_keys, cache_values)
```

```python
import jax
import jax.numpy as jnp
from jax import lax
from jax.sharding import PartitionSpec as P

D = 3584
HD = 256
WINDOW = 4096
LINE = 4

soft_cap = 50.0
norm_eps = 1e-06


def lines(axis):
    count = lax.axis_size(axis)
    return [list(range(at, at + LINE)) for at in range(0, count, LINE)]


def across_line(x):
    return lax.all_to_all(x, "seq", 0, 0, axis_index_groups=lines("seq"), tiled=True)


def swap_core(x):
    peers = lax.axis_size("tp")
    return lax.ppermute(x, "tp", [(i, i ^ 1) for i in range(peers)])


def swap_chip(x):
    peers = lax.axis_size("tp")
    return lax.ppermute(x, "tp", [(i, i ^ 2) for i in range(peers)])


def along(x, by):
    peers = lax.axis_size("seq")
    return lax.ppermute(x, "seq", [(i, i + by) for i in range(peers - by)])


def heads_first(x, heads):
    return jnp.transpose(x.reshape(x.shape[0], heads, HD), (1, 0, 2))


def ordered(is_first, mine, theirs):
    low = jnp.where(is_first, mine, theirs)
    high = jnp.where(is_first, theirs, mine)
    return jnp.concatenate([low, high], axis=0)


def attend_plane(q, k, v, mask, valid):
    scores = jnp.dot(q, k.T, preferred_element_type=jnp.float32) * HD ** (-0.5)
    capped = soft_cap * jnp.tanh(scores / soft_cap)
    weights = jnp.exp(capped)
    if mask is not None:
        weights = jnp.where(mask, weights, 0.0)
    total = jnp.sum(weights, axis=-1)
    mixture = jnp.dot(weights.astype(jnp.bfloat16), v, preferred_element_type=jnp.float32)
    if valid is not None:
        total = jnp.where(valid, total, 0.0)
    return mixture, total


def cache_rows(key_rows, value_rows, lengths, owners, position):
    rows = key_rows.shape[0]
    width = key_rows.shape[1]
    seq_devices = lax.axis_size("seq")
    spans = WINDOW // rows
    block_rows = rows // seq_devices
    row_pos = position * rows + jnp.arange(rows, dtype=jnp.int32)
    live = (row_pos < lengths[0])[:, None]
    both = jnp.concatenate([key_rows, value_rows], axis=1)
    kept = jnp.where(live, both, jnp.zeros_like(both))
    devices = jnp.arange(seq_devices, dtype=jnp.int32)
    inverse = jnp.sum(jnp.where(owners[0][:, None] == devices[None, :], devices[:, None], 0), axis=0)
    outgoing = kept.reshape(seq_devices, block_rows, 2 * width)[inverse]
    outgoing = outgoing.reshape(seq_devices, block_rows * 2 * width)
    group = position // spans
    held = jnp.where(group == 0, outgoing[:spans], jnp.zeros_like(outgoing[:spans]))
    for part in range(1, seq_devices // spans):
        sent = lax.ppermute(
            outgoing[part * spans : (part + 1) * spans],
            "seq",
            [(i, i + part * spans) for i in range(spans)],
        )
        held = jnp.where(group == part, sent, held)
    groups = [list(range(at, at + spans)) for at in range(0, seq_devices, spans)]
    got = lax.all_to_all(held, "seq", 0, 0, axis_index_groups=groups, tiled=True)
    got = got.reshape(spans * block_rows, 2 * width)
    return got[:, :width], got[:, width:]


def local(queries, key_rows, value_rows, residual, out_weight, post_scale, lengths, owners):
    rows = queries.shape[1]
    q, k, v = queries[0], key_rows[0], value_rows[0]
    position = lax.axis_index("seq")
    is_first = lax.axis_index("tp") % 2 == 0
    plane_rows = LINE * rows
    plane = position // LINE
    steps = WINDOW // plane_rows

    theirs = swap_core(jnp.where(is_first, v, k))
    mine = jnp.where(is_first, k, v)
    current = across_line(ordered(is_first, heads_first(mine, 2), heads_first(theirs, 2)))
    halves = [current[: LINE // 2].reshape(-1, HD), current[LINE // 2 :].reshape(-1, HD)]
    planes = [halves]
    for step in range(steps):
        halves = [along(half, LINE) for half in halves]
        planes.append(halves)

    pairs = q.reshape(rows, 2, 2, HD)
    even, odd = pairs[:, :, 0], pairs[:, :, 1]
    keep = jnp.transpose(jnp.where(is_first, even, odd), (1, 0, 2))
    give = jnp.transpose(jnp.where(is_first, odd, even), (1, 0, 2))
    lined = across_line(ordered(is_first, keep, swap_core(give))).reshape(plane_rows, HD)

    at = jnp.arange(plane_rows, dtype=jnp.int32)
    half_rows = plane_rows // 2
    numerator = jnp.zeros((plane_rows, HD), jnp.float32)
    denominator = jnp.zeros((plane_rows,), jnp.float32)
    for step in range(steps + 1):
        for side in range(2):
            own = planes[step][side]
            other = swap_core(own)
            keys = jnp.where(is_first, own, other)
            values = jnp.where(is_first, other, own)
            there = side * half_rows + jnp.arange(half_rows, dtype=jnp.int32)
            mask = None
            if step == 0:
                mask = at[:, None] >= there[None, :]
            if step == steps:
                mask = at[:, None] < there[None, :]
            valid = None if step == 0 else plane >= step
            mixture, total = attend_plane(lined, keys, values, mask, valid)
            numerator = numerator + mixture
            denominator = denominator + total
    attended = (numerator / denominator[:, None]).astype(jnp.bfloat16)

    back = across_line(attended.reshape(LINE, rows, HD))
    low, high = back[: LINE // 2], back[LINE // 2 :]
    theirs = swap_core(jnp.where(is_first, high, low))
    mine = jnp.where(is_first, low, high)
    head_even = jnp.where(is_first, mine, theirs)
    head_odd = jnp.where(is_first, theirs, mine)
    mixed = jnp.concatenate([head_even[0], head_odd[0], head_even[1], head_odd[1]], axis=1)

    width = out_weight.shape[1] // lax.axis_size("tp")
    partial = [
        jnp.dot(
            mixed, out_weight[:, t * width : (t + 1) * width], preferred_element_type=jnp.float32
        )
        for t in range(lax.axis_size("tp"))
    ]
    keep_0 = jnp.where(is_first, partial[0], partial[1])
    keep_1 = jnp.where(is_first, partial[2], partial[3])
    give_0 = jnp.where(is_first, partial[1], partial[0]).astype(jnp.bfloat16)
    give_1 = jnp.where(is_first, partial[3], partial[2]).astype(jnp.bfloat16)
    half_0 = keep_0 + swap_core(give_0).astype(jnp.float32)
    half_1 = keep_1 + swap_core(give_1).astype(jnp.float32)
    low_chip = lax.axis_index("tp") < 2
    kept = jnp.where(low_chip, half_0, half_1)
    given = jnp.where(low_chip, half_1, half_0).astype(jnp.bfloat16)
    branch = kept + swap_chip(given).astype(jnp.float32)
    squares = jnp.sum(branch * branch, axis=-1)
    squares = squares + swap_core(squares)
    squares = squares + swap_chip(squares)
    normed = branch * lax.rsqrt(squares / D + norm_eps)[:, None] * post_scale
    hidden_out = (residual[0].astype(jnp.float32) + normed).astype(jnp.bfloat16)

    cache_keys, cache_values = cache_rows(k, v, lengths, owners, position)
    return (hidden_out[None], cache_keys[None], cache_values[None])


def solution(mesh):
    placed = (
        P(None, "seq", "tp"),
        P(None, "seq", "tp"),
        P(None, "seq", "tp"),
        P(None, "seq", "tp"),
        P("tp", None),
        P("tp"),
        P(),
        P(),
    )
    return jax.shard_map(
        local,
        mesh=mesh,
        in_specs=placed,
        out_specs=(P(None, "seq", "tp"), P(None, "seq", "tp"), P(None, "seq", "tp")),
        check_vma=False,
    )
```

```python
import jax
import jax.numpy as jnp
from jax import lax
from jax.sharding import PartitionSpec as P

D = 3584
HD = 256
WINDOW = 4096
LINE = 4

soft_cap = 50.0
norm_eps = 1e-06


def after(x, *others):
    return lax.optimization_barrier((x, others))[0]


def swap_core(x):
    peers = lax.axis_size("tp")
    return lax.ppermute(x, "tp", [(i, i ^ 1) for i in range(peers)])


def swap_chip(x):
    peers = lax.axis_size("tp")
    return lax.ppermute(x, "tp", [(i, i ^ 2) for i in range(peers)])


def along(x, by):
    peers = lax.axis_size("seq")
    return lax.ppermute(x, "seq", [(i, i + by) for i in range(peers - by)])


def pairs_in_line(target):
    pairs = []
    for s in range(lax.axis_size("seq")):
        for t in range(lax.axis_size("tp")):
            y, core = target(s % LINE, t % 2)
            pairs.append((s * 4 + t, (s - s % LINE + y) * 4 + (t - t % 2 + core)))
    return pairs


def block_pairs(m):
    return pairs_in_line(lambda y, core: (2 * core + (m ^ (y & 1)), y >> 1))


def head_pairs(a, b):
    return pairs_in_line(lambda y, core: (2 * core + (a ^ (y & 1)), b ^ (y >> 1)))


def move(x, pairs):
    return lax.ppermute(x, ("seq", "tp"), pairs)


def head_of(x, head):
    return lax.dynamic_slice_in_dim(x, head * HD, HD, axis=1)


def regroup(x, low_bit):
    return jnp.concatenate(
        [move(head_of(x, m ^ low_bit), block_pairs(m)) for m in range(2)], axis=0
    )


def weigh(q, k, mask, valid):
    scores = lax.dot_general(
        q, k, (((1,), (1,)), ((), ())), preferred_element_type=jnp.float32
    ) * HD ** (-0.5)
    weights = jnp.exp(soft_cap * jnp.tanh(scores / soft_cap))
    if mask is not None:
        weights = jnp.where(mask, weights, 0.0)
    total = jnp.sum(weights, axis=-1)
    if valid is not None:
        total = jnp.where(valid, total, 0.0)
    return weights.astype(jnp.bfloat16), total


def pick(select, rows):
    return jnp.dot(
        select.astype(jnp.bfloat16), rows, preferred_element_type=jnp.float32
    ).astype(jnp.bfloat16)


def cache_outgoing(key_rows, value_rows, lengths, owners, position):
    rows, width = key_rows.shape
    live = (position * rows + jnp.arange(rows, dtype=jnp.int32) < lengths[0])[:, None]
    both = jnp.concatenate([key_rows, value_rows], axis=1)
    both = jnp.where(live, both, jnp.zeros_like(both))
    y, u = position % LINE, (position // LINE) % 4
    row = jnp.arange(rows, dtype=jnp.int32)
    to_y = y ^ ((row >> 6) & 3)
    to_x = (row >> 5) & 1
    far = (row >> 4) & 1
    to_z = u ^ ((row >> 2) & 3) ^ (3 * far)
    to = to_x * 32 + (far * 4 + to_z) * LINE + to_y
    block = row // (rows // owners.shape[1])
    fits = (owners[0][None, :] == to[:, None])
    number = jnp.arange(owners.shape[1], dtype=jnp.int32)
    wanted = jnp.sum(jnp.where(fits, number[None, :], 0), axis=1)
    return pick((wanted[:, None] == block[None, :]) & ((row & 3)[:, None] == (row & 3)[None, :]), both)


def cut(parts):
    at = parts[0].shape[0] // 2
    return [p[:at] for p in parts], jnp.concatenate([p[at:] for p in parts], axis=0)


def apart(x, count):
    each = x.shape[0] // count
    return [x[n * each : (n + 1) * each] for n in range(count)]


def first_planes(e):
    return [(i, i ^ e) for i in range(16)]


def cache_y1(outgoing):
    kept, given = cut([outgoing])
    return kept + [lax.ppermute(given, "seq", first_planes(2))]


def cache_y0(held):
    kept, given = cut(held)
    return kept + apart(lax.ppermute(given, "seq", first_planes(1)), 2)


def cache_x(held, position):
    kept, given = cut(held)
    got = lax.ppermute(given, "seq", [(i, i + 32) for i in range(16)])
    return jnp.where(position < 32, jnp.concatenate(kept, axis=0), got)


def cache_far(held, position):
    kept, given = cut(apart(held, 4))
    pairs = [
        (x * 32 + z * LINE + y, x * 32 + (7 - z) * LINE + y)
        for x in range(2)
        for z in range(4)
        for y in range(LINE)
    ]
    got = lax.ppermute(given, "seq", pairs)
    return jnp.where((position // LINE) % 8 < 4, jnp.concatenate(kept, axis=0), got)


def cache_w(held, e):
    kept, given = cut(held)
    got = lax.ppermute(given, "seq", [(i, i ^ (e * LINE)) for i in range(64)])
    return kept + apart(got, len(held))


def cache_turn(held):
    row = jnp.arange(64, dtype=jnp.int32)
    take = ((row >> 2) & 3) * 16 + (row >> 4) * 4 + (row & 3)
    return pick(take[:, None] == row[None, :], held)


def cache_sorted(held, position):
    z, y = (position // LINE) % 8, position % LINE
    u = jnp.where(z < 4, z, 7 - z)
    row = jnp.arange(64, dtype=jnp.int32)
    z_from = u ^ (((row >> 5) & 1) | (((row >> 4) & 1) << 1))
    y_from = y ^ (((row >> 3) & 1) | (((row >> 2) & 1) << 1))
    final = (z_from * LINE + y_from) * 4 + (row & 3)
    return pick(row[:, None] == final[None, :], held)


def local(queries, key_rows, value_rows, residual, out_weight, post_scale, lengths, owners):
    rows = queries.shape[1]
    q, k, v = queries[0], key_rows[0], value_rows[0]
    position = lax.axis_index("seq")
    tp = lax.axis_index("tp")
    core = tp % 2
    y = position % LINE
    y0, y1 = y & 1, y >> 1
    plane = position // LINE
    steps = WINDOW // (LINE * rows)

    k_raw = along(k, LINE)
    v_raw = along(v, LINE)
    messages = [(a, b) for a in range(2) for b in range(2)]
    lined = jnp.concatenate(
        [move(head_of(q, 2 * (a ^ y0) + (b ^ y1)), head_pairs(a, b)) for a, b in messages], axis=0
    )
    k_one = regroup(k_raw, y0)
    v_one = regroup(v_raw, y0)
    k_zero = regroup(after(k, k_one), y0)
    v_zero = regroup(after(v, v_one), y0)
    keys, values = [k_zero, k_one], [v_zero, v_one]
    for step in range(2, steps + 1):
        keys.append(along(keys[-1], LINE))
        values.append(along(values[-1], LINE))

    width = out_weight.shape[1] // lax.axis_size("tp")
    weight = after(out_weight, keys[2])
    weights = [
        lax.dynamic_slice_in_dim(weight, t * width, width, axis=1)
        for t in (tp ^ 3, tp ^ 2, tp ^ 1, tp)
    ]
    outgoing = cache_outgoing(k, v, lengths, owners, position)
    with jax.named_scope("cache_y1"):
        held_y1 = cache_y1(after(outgoing, keys[2]))
    with jax.named_scope("cache_y0"):
        held_y0 = cache_y0(held_y1)
    with jax.named_scope("cache_x"):
        held_x = cache_x(held_y0, position)

    offsets = jnp.arange(rows, dtype=jnp.int32)
    q_at = jnp.concatenate([(2 * (b ^ core) + (a ^ y0)) * rows + offsets for a, b in messages])
    k_at = [
        jnp.concatenate([(2 * c + (m ^ y0)) * rows + offsets for m in range(2)])
        for c in (core, 1 - core)
    ]
    numerator = jnp.zeros((LINE * rows, HD), jnp.float32)
    denominator = jnp.zeros((LINE * rows,), jnp.float32)
    for step in range(steps + 1):
        key_sides = (keys[step], swap_core(keys[step]))
        value_sides = (values[step], swap_core(values[step]))
        asked = lined
        if step == 3:
            asked, weights, held_y0 = lax.optimization_barrier((lined, weights, held_y0))
        if step == 4:
            asked = after(lined, held_x)
        for side in range(2):
            mask = None
            if step == 0:
                mask = q_at[:, None] >= k_at[side][None, :]
            if step == steps:
                mask = q_at[:, None] < k_at[side][None, :]
            rounded, total = weigh(
                asked, key_sides[side], mask, None if step == 0 else plane >= step
            )
            numerator = numerator + jnp.dot(
                rounded, value_sides[side], preferred_element_type=jnp.float32
            )
            denominator = denominator + total
    attended = (numerator / denominator[:, None]).astype(jnp.bfloat16)

    returned = {}
    for n, (a, b) in enumerate(messages):
        with jax.named_scope(f"back_{n}"):
            returned[a, b] = move(
                attended[n * rows : (n + 1) * rows],
                [(there, here) for here, there in head_pairs(a, b)],
            )
    with jax.named_scope("cache_far"):
        held_far = cache_far(after(held_x, attended), position)
    by_head = []
    for j in range(2):
        flipped = [jnp.where(y0 == 0, returned[j, b], returned[1 - j, b]) for b in range(2)]
        for b in range(2):
            by_head.append(jnp.where(y1 == 0, flipped[b], flipped[1 - b]))
    mixed = jnp.concatenate(by_head, axis=1)

    def project(w):
        return jnp.dot(mixed, w, preferred_element_type=jnp.float32)

    give_away = swap_core(project(weights[0]).astype(jnp.bfloat16))
    keep_away = project(weights[1])
    give_own = swap_core(project(weights[2]).astype(jnp.bfloat16))
    keep_own = project(weights[3])
    away = (keep_away + give_away.astype(jnp.float32)).astype(jnp.bfloat16)
    with jax.named_scope("across"):
        across = swap_chip(away)
    turned = cache_turn(after(held_far, away))
    with jax.named_scope("cache_w1"):
        held_w1 = cache_w([turned], 2)
    with jax.named_scope("cache_w0"):
        held_w0 = cache_w(held_w1, 1)
    cache = cache_sorted(jnp.concatenate(held_w0, axis=0), position)
    cache_keys, cache_values = cache[:, : k.shape[1]], cache[:, k.shape[1] :]
    branch = (keep_own + give_own.astype(jnp.float32)) + across.astype(jnp.float32)
    squares = jnp.sum(branch * branch, axis=-1)
    squares = squares + swap_core(squares)
    squares = squares + swap_chip(squares)
    normed = branch * lax.rsqrt(squares / D + norm_eps)[:, None] * post_scale
    hidden_out = (residual[0].astype(jnp.float32) + normed).astype(jnp.bfloat16)
    return (hidden_out[None], cache_keys[None], cache_values[None])


def solution(mesh):
    placed = (
        P(None, "seq", "tp"),
        P(None, "seq", "tp"),
        P(None, "seq", "tp"),
        P(None, "seq", "tp"),
        P("tp", None),
        P("tp"),
        P(),
        P(),
    )
    return jax.shard_map(
        local,
        mesh=mesh,
        in_specs=placed,
        out_specs=(P(None, "seq", "tp"), P(None, "seq", "tp"), P(None, "seq", "tp")),
        check_vma=False,
    )
```

```python
import jax
import jax.numpy as jnp
from jax import lax
from jax.sharding import PartitionSpec as P


D = 3584
HD = 256
WINDOW = 4096
LINE = 4

soft_cap = 50.0
norm_eps = 1e-06


def after(x, *others):
    return lax.optimization_barrier((x, others))[0]


def swap_core(x):
    peers = lax.axis_size("tp")
    return lax.ppermute(x, "tp", [(i, i ^ 1) for i in range(peers)])


def swap_chip(x):
    peers = lax.axis_size("tp")
    return lax.ppermute(x, "tp", [(i, i ^ 2) for i in range(peers)])


def along(x, by):
    peers = lax.axis_size("seq")
    return lax.ppermute(x, "seq", [(i, i + by) for i in range(peers - by)])


def pairs_in_line(target):
    pairs = []
    for s in range(lax.axis_size("seq")):
        for t in range(lax.axis_size("tp")):
            y, core = target(s % LINE, t % 2)
            pairs.append((s * 4 + t, (s - s % LINE + y) * 4 + (t - t % 2 + core)))
    return pairs


def block_pairs(m):
    return pairs_in_line(lambda y, core: (2 * core + (m ^ (y & 1)), y >> 1))


def head_pairs(a, b):
    return pairs_in_line(lambda y, core: (2 * core + (a ^ (y & 1)), b ^ (y >> 1)))


def move(x, pairs):
    return lax.ppermute(x, ("seq", "tp"), pairs)


def head_of(x, head):
    return lax.dynamic_slice_in_dim(x, head * HD, HD, axis=1)


def regroup(x, low_bit):
    return [move(head_of(x, m ^ low_bit), block_pairs(m)) for m in range(2)]


def weigh(q, k, mask, valid):
    scores = lax.dot_general(
        q, k, (((1,), (1,)), ((), ())), preferred_element_type=jnp.float32
    ) * HD ** (-0.5)
    weights = jnp.exp(soft_cap * jnp.tanh(scores / soft_cap))
    if mask is not None:
        weights = jnp.where(mask, weights, 0.0)
    total = jnp.sum(weights, axis=-1)
    if valid is not None:
        total = jnp.where(valid, total, 0.0)
    return weights.astype(jnp.bfloat16), total


def pick(select, rows):
    return jnp.dot(
        select.astype(jnp.bfloat16), rows, preferred_element_type=jnp.float32
    ).astype(jnp.bfloat16)


def cache_outgoing(key_rows, value_rows, lengths, owners, position):
    rows, _ = key_rows.shape
    live = (position * rows + jnp.arange(rows, dtype=jnp.int32) < lengths[0])[:, None]
    both = jnp.concatenate([key_rows, value_rows], axis=1)
    both = jnp.where(live, both, jnp.zeros_like(both))
    y, u = position % LINE, (position // LINE) % 4
    row = jnp.arange(rows, dtype=jnp.int32)
    to_x = (row >> 7) & 1
    to_y = y ^ ((row >> 5) & 3)
    far = (row >> 4) & 1
    to_z = u ^ ((row >> 2) & 3) ^ (3 * far)
    to = to_x * 32 + (far * 4 + to_z) * LINE + to_y
    block = row // (rows // owners.shape[1])
    fits = (owners[0][None, :] == to[:, None])
    number = jnp.arange(owners.shape[1], dtype=jnp.int32)
    wanted = jnp.sum(jnp.where(fits, number[None, :], 0), axis=1)
    return pick((wanted[:, None] == block[None, :]) & ((row & 3)[:, None] == (row & 3)[None, :]), both)


def cut(parts):
    at = parts[0].shape[0] // 2
    return [p[:at] for p in parts], jnp.concatenate([p[at:] for p in parts], axis=0)


def apart(x, count):
    each = x.shape[0] // count
    return [x[n * each : (n + 1) * each] for n in range(count)]


def first_planes(e):
    return [(x + i, x + (i ^ e)) for x in (0, 32) for i in range(16)]


def cache_x(outgoing, position):
    kept, given = cut([outgoing])
    got = lax.ppermute(given, "seq", [(i, i + 32) for i in range(16)])
    return jnp.where(position < 32, kept[0], got)


def cache_y1(held):
    kept, given = cut([held])
    return kept + [lax.ppermute(given, "seq", first_planes(2))]


def cache_y0(held):
    kept, given = cut(held)
    return kept + apart(lax.ppermute(given, "seq", first_planes(1)), 2)


def cache_far(held, position):
    kept, given = cut(held)
    pairs = [
        (x * 32 + z * LINE + y, x * 32 + (7 - z) * LINE + y)
        for x in range(2)
        for z in range(4)
        for y in range(LINE)
    ]
    got = lax.ppermute(given, "seq", pairs)
    return jnp.where((position // LINE) % 8 < 4, jnp.concatenate(kept, axis=0), got)


def cache_w(held, e):
    kept, given = cut(held)
    got = lax.ppermute(given, "seq", [(i, i ^ (e * LINE)) for i in range(64)])
    return kept + apart(got, len(held))


def cache_turn(held):
    row = jnp.arange(64, dtype=jnp.int32)
    take = ((row >> 2) & 3) * 16 + (row >> 4) * 4 + (row & 3)
    return pick(take[:, None] == row[None, :], held)


def cache_sorted(held, position):
    z, y = (position // LINE) % 8, position % LINE
    u = jnp.where(z < 4, z, 7 - z)
    row = jnp.arange(64, dtype=jnp.int32)
    z_from = u ^ (((row >> 5) & 1) | (((row >> 4) & 1) << 1))
    y_from = y ^ (((row >> 3) & 1) | (((row >> 2) & 1) << 1))
    final = (z_from * LINE + y_from) * 4 + (row & 3)
    return pick(row[:, None] == final[None, :], held)


def layer(queries, key_rows, value_rows, residual, out_weight, post_scale, lengths, owners):
    rows = queries.shape[1]
    q, k, v = queries[0], key_rows[0], value_rows[0]
    position = lax.axis_index("seq")
    tp = lax.axis_index("tp")
    core = tp % 2
    y = position % LINE
    y0, y1 = y & 1, y >> 1
    plane = position // LINE
    steps = WINDOW // (LINE * rows)

    k_raw = along(k, LINE)
    v_raw = along(v, LINE)
    messages = [(a, b) for b in range(2) for a in range(2)]
    asked_for = [head_of(q, 2 * (a ^ y0) + (b ^ y1)) for a, b in messages]
    stored = regroup(k_raw, y0) + regroup(v_raw, y0)
    chunks = [None, jnp.concatenate(stored, axis=0)]
    for _ in range(2, steps + 1):
        chunks.append(along(chunks[-1], LINE))
    lined = []
    for n, (a, b) in enumerate(messages):
        columns = [asked_for[n]]
        if b == 0:
            columns += [head_of(k, a ^ y0), head_of(v, a ^ y0)]
        got = move(jnp.concatenate(columns, axis=1), head_pairs(a, b))
        lined.append(got)
    chunks[0] = jnp.concatenate(
        [got[:, at : at + HD] for at in (HD, 2 * HD) for got in lined[:2]], axis=0
    )
    lined = jnp.concatenate([got[:, :HD] for got in lined], axis=0)

    width = out_weight.shape[1] // lax.axis_size("tp")
    weight = after(out_weight, chunks[3])
    weights = [
        lax.dynamic_slice_in_dim(weight, t * width, width, axis=1)
        for t in (tp ^ 3, tp ^ 2, tp ^ 1, tp)
    ]
    outgoing = cache_outgoing(k, v, lengths, owners, position)
    held_x = cache_x(outgoing, position)
    held_y1 = cache_y1(held_x)
    held_y0 = cache_y0(held_y1)

    offsets = jnp.arange(rows, dtype=jnp.int32)
    q_at = jnp.concatenate([(2 * (b ^ core) + (a ^ y0)) * rows + offsets for a, b in messages])
    k_at = [
        jnp.concatenate([(2 * c + (m ^ y0)) * rows + offsets for m in range(2)])
        for c in (core, 1 - core)
    ]
    numerator = jnp.zeros((LINE * rows, HD), jnp.float32)
    denominator = jnp.zeros((LINE * rows,), jnp.float32)
    for step in range(steps + 1):
        sides = [chunks[step], swap_core(chunks[step])]
        asked = lined
        if step == steps:
            asked, weights = lax.optimization_barrier((lined, weights))
            numerator = lax.optimization_barrier(numerator)
        for side, chunk in enumerate(sides):
            mask = None
            if step == 0:
                mask = q_at[:, None] >= k_at[side][None, :]
            if step == steps:
                mask = q_at[:, None] < k_at[side][None, :]
            rounded, total = weigh(
                asked, chunk[: 2 * rows], mask, None if step == 0 else plane >= step
            )
            numerator = numerator + jnp.dot(
                rounded, chunk[2 * rows :], preferred_element_type=jnp.float32
            )
            denominator = denominator + total
    attended = (numerator / denominator[:, None]).astype(jnp.bfloat16)

    returned = {}
    for n, (a, b) in enumerate(messages):
        returned[a, b] = move(
            attended[n * rows : (n + 1) * rows],
            [(there, here) for here, there in head_pairs(a, b)],
        )
    held_far = cache_far(after(held_y0, attended), position)
    by_head = []
    for j in range(2):
        flipped = [jnp.where(y0 == 0, returned[j, b], returned[1 - j, b]) for b in range(2)]
        for b in range(2):
            by_head.append(jnp.where(y1 == 0, flipped[b], flipped[1 - b]))
    mixed = jnp.concatenate(by_head, axis=1)

    def project(w):
        return jnp.dot(mixed, w, preferred_element_type=jnp.float32)

    give_away = swap_core(project(weights[0]).astype(jnp.bfloat16))
    keep_away = project(weights[1])
    give_own = swap_core(project(weights[2]).astype(jnp.bfloat16))
    keep_own = project(weights[3])
    away = (keep_away + give_away.astype(jnp.float32)).astype(jnp.bfloat16)
    across = swap_chip(away)
    turned = cache_turn(after(held_far, away))
    held_w1 = cache_w([turned], 2)
    held_w0 = cache_w(held_w1, 1)
    cache = cache_sorted(jnp.concatenate(held_w0, axis=0), position)
    cache_keys, cache_values = cache[:, : k.shape[1]], cache[:, k.shape[1] :]
    branch = (keep_own + give_own.astype(jnp.float32)) + across.astype(jnp.float32)
    squares = jnp.sum(branch * branch, axis=-1)
    squares = squares + swap_core(squares)
    squares = squares + swap_chip(squares)
    normed = branch * lax.rsqrt(squares / D + norm_eps)[:, None] * post_scale
    hidden_out = (residual[0].astype(jnp.float32) + normed).astype(jnp.bfloat16)
    return (hidden_out[None], cache_keys[None], cache_values[None])


def solution(mesh):
    placed = (
        P(None, "seq", "tp"),
        P(None, "seq", "tp"),
        P(None, "seq", "tp"),
        P(None, "seq", "tp"),
        P("tp", None),
        P("tp"),
        P(),
        P(),
    )
    return jax.shard_map(
        layer,
        mesh=mesh,
        in_specs=placed,
        out_specs=(P(None, "seq", "tp"), P(None, "seq", "tp"), P(None, "seq", "tp")),
        check_vma=False,
    )
```

```python
import jax
import jax.numpy as jnp
from jax import lax
from jax.sharding import PartitionSpec as P


D = 3584
HD = 256
WINDOW = 4096
LINE = 4

soft_cap = 50.0
norm_eps = 1e-06


def after(x, *others):
    return lax.optimization_barrier((x, others))[0]


def swap_core(x):
    peers = lax.axis_size("tp")
    return lax.ppermute(x, "tp", [(i, i ^ 1) for i in range(peers)])


def swap_chip(x):
    peers = lax.axis_size("tp")
    return lax.ppermute(x, "tp", [(i, i ^ 2) for i in range(peers)])


def along(x, by):
    peers = lax.axis_size("seq")
    return lax.ppermute(x, "seq", [(i, i + by) for i in range(peers - by)])


def pairs_in_line(target):
    pairs = []
    for s in range(lax.axis_size("seq")):
        for t in range(lax.axis_size("tp")):
            y, core = target(s % LINE, t % 2)
            pairs.append((s * 4 + t, (s - s % LINE + y) * 4 + (t - t % 2 + core)))
    return pairs


def block_pairs(m):
    return pairs_in_line(lambda y, core: (2 * core + (m ^ (y & 1)), y >> 1))


def head_pairs(a, b):
    return pairs_in_line(lambda y, core: (2 * core + (a ^ (y & 1)), b ^ (y >> 1)))


def move(x, pairs):
    return lax.ppermute(x, ("seq", "tp"), pairs)


def head_of(x, head):
    return lax.dynamic_slice_in_dim(x, head * HD, HD, axis=1)


def regroup(x, low_bit):
    return [move(head_of(x, m ^ low_bit), block_pairs(m)) for m in range(2)]


def weigh(q, k, mask, valid):
    scores = lax.dot_general(
        q, k, (((1,), (1,)), ((), ())), preferred_element_type=jnp.float32
    ) * HD ** (-0.5)
    weights = jnp.exp(soft_cap * jnp.tanh(scores / soft_cap))
    if mask is not None:
        weights = jnp.where(mask, weights, 0.0)
    total = jnp.sum(weights, axis=-1)
    if valid is not None:
        total = jnp.where(valid, total, 0.0)
    return weights.astype(jnp.bfloat16), total


def pick(select, rows):
    return jnp.dot(
        select.astype(jnp.bfloat16), rows, preferred_element_type=jnp.float32
    ).astype(jnp.bfloat16)


def cache_outgoing(key_rows, value_rows, lengths, owners, position):
    rows, _ = key_rows.shape
    live = (position * rows + jnp.arange(rows, dtype=jnp.int32) < lengths[0])[:, None]
    both = jnp.concatenate([key_rows, value_rows], axis=1)
    both = jnp.where(live, both, jnp.zeros_like(both))
    y, u = position % LINE, (position // LINE) % 4
    row = jnp.arange(rows, dtype=jnp.int32)
    to_x = (row >> 7) & 1
    to_y = y ^ ((row >> 5) & 3)
    far = (row >> 4) & 1
    to_z = u ^ ((row >> 2) & 3) ^ (3 * far)
    to = to_x * 32 + (far * 4 + to_z) * LINE + to_y
    block = row // (rows // owners.shape[1])
    fits = (owners[0][None, :] == to[:, None])
    number = jnp.arange(owners.shape[1], dtype=jnp.int32)
    wanted = jnp.sum(jnp.where(fits, number[None, :], 0), axis=1)
    return pick((wanted[:, None] == block[None, :]) & ((row & 3)[:, None] == (row & 3)[None, :]), both)


def cut(parts):
    at = parts[0].shape[0] // 2
    return [p[:at] for p in parts], jnp.concatenate([p[at:] for p in parts], axis=0)


def apart(x, count):
    each = x.shape[0] // count
    return [x[n * each : (n + 1) * each] for n in range(count)]


def first_planes(e):
    return [(x + i, x + (i ^ e)) for x in (0, 32) for i in range(16)]


def cache_x(outgoing, position):
    kept, given = cut([outgoing])
    got = lax.ppermute(given, "seq", [(i, i + 32) for i in range(16)])
    return jnp.where(position < 32, kept[0], got)


def cache_y1(held):
    kept, given = cut([held])
    return kept + [lax.ppermute(given, "seq", first_planes(2))]


def cache_y0(held):
    kept, given = cut(held)
    return kept + apart(lax.ppermute(given, "seq", first_planes(1)), 2)


def cache_far(held, position):
    kept, given = cut(held)
    pairs = [
        (x * 32 + z * LINE + y, x * 32 + (7 - z) * LINE + y)
        for x in range(2)
        for z in range(4)
        for y in range(LINE)
    ]
    got = lax.ppermute(given, "seq", pairs)
    return jnp.where((position // LINE) % 8 < 4, jnp.concatenate(kept, axis=0), got)


def cache_w(held, e):
    kept, given = cut(held)
    got = lax.ppermute(given, "seq", [(i, i ^ (e * LINE)) for i in range(64)])
    return kept + apart(got, len(held))


def cache_turn(held):
    row = jnp.arange(64, dtype=jnp.int32)
    take = ((row >> 2) & 3) * 16 + (row >> 4) * 4 + (row & 3)
    return pick(take[:, None] == row[None, :], held)


def cache_sorted(held, position):
    z, y = (position // LINE) % 8, position % LINE
    u = jnp.where(z < 4, z, 7 - z)
    row = jnp.arange(64, dtype=jnp.int32)
    z_from = u ^ (((row >> 5) & 1) | (((row >> 4) & 1) << 1))
    y_from = y ^ (((row >> 3) & 1) | (((row >> 2) & 1) << 1))
    final = (z_from * LINE + y_from) * 4 + (row & 3)
    return pick(row[:, None] == final[None, :], held)


def layer(queries, key_rows, value_rows, residual, out_weight, post_scale, lengths, owners):
    rows = queries.shape[1]
    q, k, v = queries[0], key_rows[0], value_rows[0]
    position = lax.axis_index("seq")
    tp = lax.axis_index("tp")
    core = tp % 2
    y = position % LINE
    y0, y1 = y & 1, y >> 1
    plane = position // LINE
    steps = WINDOW // (LINE * rows)

    k_raw = along(k, LINE)
    v_raw = along(v, LINE)
    messages = [(a, b) for b in range(2) for a in range(2)]
    asked_for = [head_of(q, 2 * (a ^ y0) + (b ^ y1)) for a, b in messages]
    stored = regroup(k_raw, y0) + regroup(v_raw, y0)
    chunks = [None, jnp.concatenate(stored, axis=0)]
    for _ in range(2, steps + 1):
        chunks.append(along(chunks[-1], LINE))
    lined = []
    for n, (a, b) in enumerate(messages):
        columns = [asked_for[n]]
        if b == 0:
            columns += [head_of(k, a ^ y0), head_of(v, a ^ y0)]
        got = move(jnp.concatenate(columns, axis=1), head_pairs(a, b))
        lined.append(got)
    chunks[0] = jnp.concatenate(
        [got[:, at : at + HD] for at in (HD, 2 * HD) for got in lined[:2]], axis=0
    )
    lined = jnp.concatenate([got[:, :HD] for got in lined], axis=0)

    width = out_weight.shape[1] // lax.axis_size("tp")
    outgoing = cache_outgoing(k, v, lengths, owners, position)
    held_x = cache_x(outgoing, position)
    held_y1 = cache_y1(held_x)
    held_y0 = cache_y0(held_y1)

    offsets = jnp.arange(rows, dtype=jnp.int32)
    q_at = jnp.concatenate([(2 * (b ^ core) + (a ^ y0)) * rows + offsets for a, b in messages])
    k_at = [
        jnp.concatenate([(2 * c + (m ^ y0)) * rows + offsets for m in range(2)])
        for c in (core, 1 - core)
    ]
    numerator = jnp.zeros((LINE * rows, HD), jnp.float32)
    denominator = jnp.zeros((LINE * rows,), jnp.float32)
    for step in (1, 0, 2, 3, 4):
        sides = [chunks[step], swap_core(chunks[step])]
        asked = lined
        if step != 1:
            numerator = lax.optimization_barrier(numerator)
        for side, chunk in enumerate(sides):
            mask = None
            if step == 0:
                mask = q_at[:, None] >= k_at[side][None, :]
            if step == steps:
                mask = q_at[:, None] < k_at[side][None, :]
            rounded, total = weigh(
                asked, chunk[: 2 * rows], mask, None if step == 0 else plane >= step
            )
            numerator = numerator + jnp.dot(
                rounded, chunk[2 * rows :], preferred_element_type=jnp.float32
            )
            denominator = denominator + total
    attended = (numerator / denominator[:, None]).astype(jnp.bfloat16)

    returned = {}
    for n, (a, b) in enumerate(messages):
        returned[a, b] = move(
            attended[n * rows : (n + 1) * rows],
            [(there, here) for here, there in head_pairs(a, b)],
        )
    held_far = cache_far(after(held_y0, attended), position)
    by_head = []
    for j in range(2):
        flipped = [jnp.where(y0 == 0, returned[j, b], returned[1 - j, b]) for b in range(2)]
        for b in range(2):
            by_head.append(jnp.where(y1 == 0, flipped[b], flipped[1 - b]))
    mixed = jnp.concatenate(by_head, axis=1)

    partial = jnp.dot(mixed, out_weight, preferred_element_type=jnp.float32)
    partial = partial.astype(jnp.bfloat16)

    def part(t):
        return lax.dynamic_slice_in_dim(partial, t * width, width, axis=1)

    give_away = swap_core(part(tp ^ 3))
    give_own = swap_core(part(tp ^ 1))
    away = (part(tp ^ 2).astype(jnp.float32) + give_away.astype(jnp.float32)).astype(jnp.bfloat16)
    keep_own = part(tp).astype(jnp.float32)
    across = swap_chip(away)
    turned = cache_turn(after(held_far, away))
    held_w1 = cache_w([turned], 2)
    held_w0 = cache_w(held_w1, 1)
    cache = cache_sorted(jnp.concatenate(held_w0, axis=0), position)
    cache_keys, cache_values = cache[:, : k.shape[1]], cache[:, k.shape[1] :]
    branch = (keep_own + give_own.astype(jnp.float32)) + across.astype(jnp.float32)
    squares = jnp.sum(branch * branch, axis=-1)
    squares = squares + swap_core(squares)
    squares = squares + swap_chip(squares)
    normed = branch * lax.rsqrt(squares / D + norm_eps)[:, None] * post_scale
    hidden_out = (residual[0].astype(jnp.float32) + normed).astype(jnp.bfloat16)
    return (hidden_out[None], cache_keys[None], cache_values[None])


def solution(mesh):
    placed = (
        P(None, "seq", "tp"),
        P(None, "seq", "tp"),
        P(None, "seq", "tp"),
        P(None, "seq", "tp"),
        P("tp", None),
        P("tp"),
        P(),
        P(),
    )
    return jax.shard_map(
        layer,
        mesh=mesh,
        in_specs=placed,
        out_specs=(P(None, "seq", "tp"), P(None, "seq", "tp"), P(None, "seq", "tp")),
        check_vma=False,
    )
```

```python
import jax
import jax.numpy as jnp
from jax import lax
from jax.sharding import PartitionSpec as P


D = 3584
HD = 256
WINDOW = 4096
LINE = 4

soft_cap = 50.0
norm_eps = 1e-06


def after(x, *others):
    return lax.optimization_barrier((x, others))[0]


def swap_core(x):
    peers = lax.axis_size("tp")
    return lax.ppermute(x, "tp", [(i, i ^ 1) for i in range(peers)])


def swap_chip(x):
    peers = lax.axis_size("tp")
    return lax.ppermute(x, "tp", [(i, i ^ 2) for i in range(peers)])


def along(x, by):
    peers = lax.axis_size("seq")
    return lax.ppermute(x, "seq", [(i, i + by) for i in range(peers - by)])


def pairs_in_line(target):
    pairs = []
    for s in range(lax.axis_size("seq")):
        for t in range(lax.axis_size("tp")):
            y, core = target(s % LINE, t % 2)
            pairs.append((s * 4 + t, (s - s % LINE + y) * 4 + (t - t % 2 + core)))
    return pairs


def block_pairs(m):
    return pairs_in_line(lambda y, core: (2 * core + (m ^ (y & 1)), y >> 1))


def head_pairs(a, b):
    return pairs_in_line(lambda y, core: (2 * core + (a ^ (y & 1)), b ^ (y >> 1)))


def move(x, pairs):
    return lax.ppermute(x, ("seq", "tp"), pairs)


def head_of(x, head):
    return lax.dynamic_slice_in_dim(x, head * HD, HD, axis=1)


def regroup(x, low_bit):
    return [move(head_of(x, m ^ low_bit), block_pairs(m)) for m in range(2)]


def weigh(q, k, mask, valid):
    scores = lax.dot_general(
        q, k, (((1,), (1,)), ((), ())), preferred_element_type=jnp.float32
    ) * HD ** (-0.5)
    weights = jnp.exp(soft_cap * jnp.tanh(scores / soft_cap))
    if mask is not None:
        weights = jnp.where(mask, weights, 0.0)
    total = jnp.sum(weights, axis=-1)
    if valid is not None:
        total = jnp.where(valid, total, 0.0)
    return weights.astype(jnp.bfloat16), total


def pick(select, rows):
    return jnp.dot(
        select.astype(jnp.bfloat16), rows, preferred_element_type=jnp.float32
    ).astype(jnp.bfloat16)


def cache_outgoing(key_rows, value_rows, lengths, owners, position):
    rows, _ = key_rows.shape
    live = (position * rows + jnp.arange(rows, dtype=jnp.int32) < lengths[0])[:, None]
    both = jnp.concatenate([key_rows, value_rows], axis=1)
    both = jnp.where(live, both, jnp.zeros_like(both))
    y, u = position % LINE, (position // LINE) % 4
    row = jnp.arange(rows, dtype=jnp.int32)
    to_x = (row >> 7) & 1
    to_y = y ^ ((row >> 5) & 3)
    far = (row >> 4) & 1
    to_z = u ^ ((row >> 2) & 3) ^ (3 * far)
    to = to_x * 32 + (far * 4 + to_z) * LINE + to_y
    block = row // (rows // owners.shape[1])
    fits = (owners[0][None, :] == to[:, None])
    number = jnp.arange(owners.shape[1], dtype=jnp.int32)
    wanted = jnp.sum(jnp.where(fits, number[None, :], 0), axis=1)
    return pick((wanted[:, None] == block[None, :]) & ((row & 3)[:, None] == (row & 3)[None, :]), both)


def cut(parts):
    at = parts[0].shape[0] // 2
    return [p[:at] for p in parts], jnp.concatenate([p[at:] for p in parts], axis=0)


def apart(x, count):
    each = x.shape[0] // count
    return [x[n * each : (n + 1) * each] for n in range(count)]


def first_planes(e):
    return [(x + i, x + (i ^ e)) for x in (0, 32) for i in range(16)]


def cache_x(outgoing, position):
    kept, given = cut([outgoing])
    got = lax.ppermute(given, "seq", [(i, i + 32) for i in range(16)])
    return jnp.where(position < 32, kept[0], got)


def cache_y1(held):
    kept, given = cut([held])
    return kept + [lax.ppermute(given, "seq", first_planes(2))]


def cache_y0(held):
    kept, given = cut(held)
    return kept + apart(lax.ppermute(given, "seq", first_planes(1)), 2)


def cache_far(held, position):
    kept, given = cut(held)
    pairs = [
        (x * 32 + z * LINE + y, x * 32 + (7 - z) * LINE + y)
        for x in range(2)
        for z in range(4)
        for y in range(LINE)
    ]
    got = lax.ppermute(given, "seq", pairs)
    return jnp.where((position // LINE) % 8 < 4, jnp.concatenate(kept, axis=0), got)


def cache_w(held, e):
    kept, given = cut(held)
    got = lax.ppermute(given, "seq", [(i, i ^ (e * LINE)) for i in range(64)])
    return kept + apart(got, len(held))


def cache_turn(held):
    row = jnp.arange(64, dtype=jnp.int32)
    take = ((row >> 2) & 3) * 16 + (row >> 4) * 4 + (row & 3)
    return pick(take[:, None] == row[None, :], held)


def cache_sorted(held, position):
    z, y = (position // LINE) % 8, position % LINE
    u = jnp.where(z < 4, z, 7 - z)
    row = jnp.arange(64, dtype=jnp.int32)
    z_from = u ^ (((row >> 5) & 1) | (((row >> 4) & 1) << 1))
    y_from = y ^ (((row >> 3) & 1) | (((row >> 2) & 1) << 1))
    final = (z_from * LINE + y_from) * 4 + (row & 3)
    return pick(row[:, None] == final[None, :], held)


def layer(queries, key_rows, value_rows, residual, out_weight, post_scale, lengths, owners):
    rows = queries.shape[1]
    q, k, v = queries[0], key_rows[0], value_rows[0]
    position = lax.axis_index("seq")
    tp = lax.axis_index("tp")
    core = tp % 2
    y = position % LINE
    y0, y1 = y & 1, y >> 1
    plane = position // LINE
    steps = WINDOW // (LINE * rows)

    k_raw = along(k, LINE)
    v_raw = along(v, LINE)
    messages = [(a, b) for b in range(2) for a in range(2)]
    asked_for = [head_of(q, 2 * (a ^ y0) + (b ^ y1)) for a, b in messages]
    keys = [None, jnp.concatenate(regroup(k_raw, y0), axis=0)]
    values = [None, jnp.concatenate(regroup(v_raw, y0), axis=0)]
    for _ in range(2, steps + 1):
        keys.append(along(keys[-1], LINE))
        values.append(along(values[-1], LINE))
    lined = []
    for n, (a, b) in enumerate(messages):
        columns = [asked_for[n]]
        if b == 0:
            columns += [head_of(k, a ^ y0), head_of(v, a ^ y0)]
        got = move(jnp.concatenate(columns, axis=1), head_pairs(a, b))
        lined.append(got)
    chunk = jnp.concatenate(
        [got[:, at : at + HD] for at in (HD, 2 * HD) for got in lined[:2]], axis=0
    )
    lined = jnp.concatenate([got[:, :HD] for got in lined], axis=0)

    width = out_weight.shape[1] // lax.axis_size("tp")
    outgoing = cache_outgoing(k, v, lengths, owners, position)
    held_x = cache_x(outgoing, position)
    held_y1 = cache_y1(held_x)
    held_y0 = cache_y0(held_y1)

    offsets = jnp.arange(rows, dtype=jnp.int32)
    q_at = jnp.concatenate([(2 * (b ^ core) + (a ^ y0)) * rows + offsets for a, b in messages])
    k_at = [
        jnp.concatenate([(2 * c + (m ^ y0)) * rows + offsets for m in range(2)])
        for c in (core, 1 - core)
    ]
    numerator = jnp.zeros((LINE * rows, HD), jnp.float32)
    denominator = jnp.zeros((LINE * rows,), jnp.float32)
    for step in (1, 0, 2, 3, 4):
        if step == 0:
            other = swap_core(chunk)
            sides = [(x[: 2 * rows], x[2 * rows :]) for x in (chunk, other)]
        else:
            sides = [
                (keys[step], values[step]),
                (swap_core(keys[step]), swap_core(values[step])),
            ]
        asked = lined
        if step != 1:
            numerator = lax.optimization_barrier(numerator)
        for side, (key_side, value_side) in enumerate(sides):
            mask = None
            if step == 0:
                mask = q_at[:, None] >= k_at[side][None, :]
            if step == steps:
                mask = q_at[:, None] < k_at[side][None, :]
            rounded, total = weigh(
                asked, key_side, mask, None if step == 0 else plane >= step
            )
            numerator = numerator + jnp.dot(
                rounded, value_side, preferred_element_type=jnp.float32
            )
            denominator = denominator + total
    attended = (numerator / denominator[:, None]).astype(jnp.bfloat16)

    returned = {}
    for n, (a, b) in enumerate(messages):
        returned[a, b] = move(
            attended[n * rows : (n + 1) * rows],
            [(there, here) for here, there in head_pairs(a, b)],
        )
    held_far = cache_far(after(held_y0, attended), position)
    by_head = []
    for j in range(2):
        flipped = [jnp.where(y0 == 0, returned[j, b], returned[1 - j, b]) for b in range(2)]
        for b in range(2):
            by_head.append(jnp.where(y1 == 0, flipped[b], flipped[1 - b]))
    mixed = jnp.concatenate(by_head, axis=1)

    partial = jnp.dot(mixed, out_weight, preferred_element_type=jnp.float32)
    partial = partial.astype(jnp.bfloat16)

    def part(t):
        return lax.dynamic_slice_in_dim(partial, t * width, width, axis=1)

    give_away = swap_core(part(tp ^ 3))
    give_own = swap_core(part(tp ^ 1))
    away = (part(tp ^ 2).astype(jnp.float32) + give_away.astype(jnp.float32)).astype(jnp.bfloat16)
    keep_own = part(tp).astype(jnp.float32)
    across = swap_chip(away)
    turned = cache_turn(after(held_far, away))
    held_w1 = cache_w([turned], 2)
    held_w0 = cache_w(held_w1, 1)
    cache = cache_sorted(jnp.concatenate(held_w0, axis=0), position)
    cache_keys, cache_values = cache[:, : k.shape[1]], cache[:, k.shape[1] :]
    branch = (keep_own + give_own.astype(jnp.float32)) + across.astype(jnp.float32)
    squares = jnp.sum(branch * branch, axis=-1)
    squares = squares + swap_core(squares)
    squares = squares + swap_chip(squares)
    normed = branch * lax.rsqrt(squares / D + norm_eps)[:, None] * post_scale
    hidden_out = (residual[0].astype(jnp.float32) + normed).astype(jnp.bfloat16)
    return (hidden_out[None], cache_keys[None], cache_values[None])


def solution(mesh):
    placed = (
        P(None, "seq", "tp"),
        P(None, "seq", "tp"),
        P(None, "seq", "tp"),
        P(None, "seq", "tp"),
        P("tp", None),
        P("tp"),
        P(),
        P(),
    )
    return jax.shard_map(
        layer,
        mesh=mesh,
        in_specs=placed,
        out_specs=(P(None, "seq", "tp"), P(None, "seq", "tp"), P(None, "seq", "tp")),
        check_vma=False,
    )
```
